16 devices in a mesh: dp: 4 (over y, z, core), sp: 4 (over x).
Axes of the slice: x: 4, y: 2, z: 1, core: 2. Of those that a mesh axis runs over, the one named last changes fastest.
The devices are a block of a 4x4x8 slice.
Arguments:
- x: bfloat16 [8192, 7168], P(('dp', 'sp')), parts along dimension 0
- gain: bfloat16 [7168], replicated
- wq: bfloat16 [7168, 7168], replicated
- wk: bfloat16 [7168, 7168], replicated
- wv: bfloat16 [7168, 7168], replicated
- wo: bfloat16 [7168, 7168], replicated
Outputs:
- output: bfloat16 [8192, 7168], P(('dp', 'sp')), parts along dimension 0
There are 4 independent parts. The reference program is written for one: setup_inputs(seed, part) draws one part's arguments, and reference() takes and returns one part's arrays. A program takes and returns all parts, laid end to end along the dimension named above; an argument that names none is the same for every part.
All inputs are finite; a program needn't handle non-finite values.
Results may differ from the reference program's by a relative error of at most 0.012.
Values are sent between devices in bfloat16 or wider.
A program may use at most 768 MiB of HBM per device.

```python
import jax
import jax.numpy as jnp
from jax import lax

ROWS = 2048
D = 7168
HEADS = 56
KV_HEADS = 56
HEAD = 128
THETA = 10000


def setup_inputs(seed: int = 0, part: int = 0) -> dict:
    kx, kn, kq, kk, kv, ko = jax.random.split(jax.random.key(seed), 6)

    def weights(key, rows, columns):
        return jax.random.normal(key, (rows, columns), jnp.float32) * rows**-0.5

    drawn = {
        "x": jax.random.normal(jax.random.fold_in(kx, part), (ROWS, D), jnp.float32),
        "gain": 1 + 0.1 * jax.random.normal(kn, (D,), jnp.float32),
        "wq": 2 * weights(kq, D, HEADS * HEAD),
        "wk": 2 * weights(kk, D, KV_HEADS * HEAD),
        "wv": 4 * weights(kv, D, KV_HEADS * HEAD),
        "wo": weights(ko, HEADS * HEAD, D),
    }
    return {k: v.astype(jnp.bfloat16) for k, v in drawn.items()}


def normed(x, gain):
    wide = x.astype(jnp.float32)
    scale = lax.rsqrt(jnp.mean(wide * wide, -1, keepdims=True) + 1e-6)
    return (wide * scale * gain.astype(jnp.float32)).astype(jnp.bfloat16)


def turned(t, place, theta):
    half = t.shape[-1] // 2
    angle = place.astype(jnp.float32)[:, None] * theta ** (-jnp.arange(half, dtype=jnp.float32) / half)
    cos, sin = jnp.cos(angle)[:, None], jnp.sin(angle)[:, None]
    a, b = t[..., :half].astype(jnp.float32), t[..., half:].astype(jnp.float32)
    return jnp.concatenate([a * cos - b * sin, b * cos + a * sin], -1).astype(jnp.bfloat16)


def matmul(a, w):
    return jnp.dot(a, w, preferred_element_type=jnp.float32).astype(jnp.bfloat16)


def einsum(form, a, b):
    return jnp.einsum(form, a.astype(jnp.float32), b.astype(jnp.float32))


def attention(q, k, v):
    scores = einsum("tgsd,ugd->gstu", q, k) * q.shape[-1] ** -0.5
    token = jnp.arange(q.shape[0])
    scores = jnp.where(token[:, None] >= token, scores, -jnp.inf)
    weights = jax.nn.softmax(scores, -1).astype(jnp.bfloat16)
    return einsum("gstu,ugd->tgsd", weights, v).astype(jnp.bfloat16)


def reference(x, gain, wq, wk, wv, wo):
    a, place = normed(x, gain), jnp.arange(ROWS)
    q = turned(matmul(a, wq).reshape(ROWS, HEADS, HEAD), place, THETA).reshape(ROWS, KV_HEADS, -1, HEAD)
    k = turned(matmul(a, wk).reshape(ROWS, KV_HEADS, HEAD), place, THETA)
    v = matmul(a, wv).reshape(ROWS, KV_HEADS, HEAD)
    seen = attention(q, k, v).reshape(ROWS, HEADS * HEAD)
    return (x.astype(jnp.float32) + jnp.dot(seen, wo, preferred_element_type=jnp.float32)).astype(jnp.bfloat16)
```

```python
import functools

import jax
import jax.numpy as jnp
from jax import lax
from jax.experimental import pallas as pl
from jax.experimental.pallas import tpu as pltpu
from jax.sharding import PartitionSpec as P

HEAD = 128
THETA = 10000
NEG = -1e30
HIDDEN = 2 * NEG
LOG2E = 1.4426950408889634
PAIR = 2
TILE = PAIR * HEAD
NW = 3
ROWS = 16
MESH = pl.DeviceIdType.MESH
Q, K = 0, 1


def _dot(a, b, ca, cb):
    return lax.dot_general(a, b, (((ca,), (cb,)), ((), ())), preferred_element_type=jnp.float32)


def _kernel(n, pairs, x_ref, gain_ref, cos_ref, sin_ref, wq, wk, wv, wo, y_ref, qk_ref, vt_ref,
            a, acc, wbuf, qk_out, vt_out, o_out, o_in, qk_in, vt_in, top_s, mix_s,
            w_sem, x_sem, y_sem, in_sem, qk_send, vt_send, o_send, qk_recv, vt_recv, o_recv):
    own, d = a.shape
    me = lax.axis_index("sp")
    wide = d // TILE
    per_step = wide // n
    depth = n * TILE
    n_qk, n_vt = 2 * n, n
    tiles = n_qk + n_vt
    proj_steps = pairs * tiles
    steps = proj_steps + pairs * n
    half = own // 2

    def column(owner, p):
        return pl.multiple_of((owner * pairs + p) * TILE, TILE)

    def owner_of(t):
        return lax.rem(me + lax.rem(t, n) + 1, n)

    def fetch(s):
        slot = lax.rem(s, NW)

        @pl.when(s < proj_steps)
        def _():
            p, t = lax.div(s, tiles), lax.rem(s, tiles)
            cols = pl.ds(column(owner_of(t), p), TILE)
            for i, w in enumerate((wq, wk, wv)):
                @pl.when(lax.div(t, n) == i)
                def _():
                    pltpu.make_async_copy(w.at[:, cols], wbuf.at[slot], w_sem.at[slot]).start()

        @pl.when((s >= proj_steps) & (s < steps))
        def _():
            p, part = lax.div(s - proj_steps, n), lax.rem(s - proj_steps, n)

            def one(c, _):
                cols = pl.ds(pl.multiple_of((part * per_step + c) * TILE, TILE), TILE)
                for owner in range(n):
                    pltpu.make_async_copy(wo.at[pl.ds(column(owner, p), TILE), cols],
                                          wbuf.at[slot, pl.ds(pl.multiple_of(c * depth + owner * TILE, TILE), TILE), :], w_sem.at[slot]).start()
                return 0

            lax.fori_loop(0, per_step, one, 0)

    def weights_here(s):
        slot = lax.rem(s, NW)
        pltpu.make_async_copy(wbuf.at[slot], wbuf.at[slot], w_sem.at[slot]).wait()
        return slot

    barrier = pltpu.get_barrier_semaphore()
    for r in range(1, n):
        pl.semaphore_signal(barrier, inc=1, device_id={"sp": lax.rem(me + r, n)}, device_id_type=MESH)
    pltpu.make_async_copy(x_ref, a, x_sem).start()
    for s in range(NW):
        fetch(jnp.int32(s))
    pltpu.make_async_copy(x_ref, a, x_sem).wait()

    def norm(i, _):
        rows = pl.ds(pl.multiple_of(i * ROWS, ROWS), ROWS)
        xr = a[rows, :].astype(jnp.float32)
        acc[rows, :] = xr
        scale = lax.rsqrt(jnp.mean(xr * xr, -1, keepdims=True) + 1e-6)
        a[rows, :] = (xr * scale * gain_ref[...]).astype(jnp.bfloat16)
        return 0

    lax.fori_loop(0, own // ROWS, norm, 0)
    pl.semaphore_wait(barrier, n - 1)

    def tile_of(s):
        slot = weights_here(s)
        t = jnp.dot(a[...], wbuf[slot], preferred_element_type=jnp.float32).astype(jnp.bfloat16)
        fetch(s + NW)
        return t

    mine = pl.ds(pl.multiple_of(me * own, own), own)

    def project_qk(p, t):
        tile = tile_of(p * tiles + t)
        m, owner, use = lax.div(t, n), owner_of(t), p * n_qk + t
        slot = lax.rem(use, 2 * n_qk)
        away = owner != me

        @pl.when(away & (use >= 2 * n_qk))
        def _():
            pltpu.make_async_copy(qk_out.at[slot], qk_out.at[slot], qk_send.at[slot]).wait()

        for h in range(PAIR):
            one = tile[:, h * HEAD : (h + 1) * HEAD].astype(jnp.float32)
            turned = one * cos_ref[...] + pltpu.roll(one, HEAD // 2, 1) * sin_ref[...]
            qk_out[slot, h] = turned.astype(jnp.bfloat16)

        @pl.when(away)
        def _():
            pltpu.make_async_remote_copy(qk_out.at[slot], qk_ref.at[p, m, :, mine, :], qk_send.at[slot], qk_recv.at[p],
                                         device_id={"sp": owner}, device_id_type=MESH).start()

        @pl.when(jnp.logical_not(away))
        def _():
            pltpu.make_async_copy(qk_out.at[slot], qk_ref.at[p, m, :, mine, :], qk_recv.at[p]).start()

    def project_vt(p, t):
        tile = tile_of(p * tiles + t)
        owner, use = owner_of(t), p * n_vt + t - n_qk
        slot = lax.rem(use, 2 * n_vt)
        away = owner != me

        @pl.when(away & (use >= 2 * n_vt))
        def _():
            pltpu.make_async_copy(vt_out.at[slot], vt_out.at[slot], vt_send.at[slot]).wait()

        for h in range(PAIR):
            vt_out[slot, h] = tile[:, h * HEAD : (h + 1) * HEAD].T

        @pl.when(away)
        def _():
            pltpu.make_async_remote_copy(vt_out.at[slot], vt_ref.at[p, :, :, mine], vt_send.at[slot], vt_recv.at[p],
                                         device_id={"sp": owner}, device_id_type=MESH).start()

        @pl.when(jnp.logical_not(away))
        def _():
            pltpu.make_async_copy(vt_out.at[slot], vt_ref.at[p, :, :, mine], vt_recv.at[p]).start()

    def load_pair(p):
        pltpu.make_async_copy(qk_ref.at[p], qk_ref.at[p], qk_recv.at[p]).wait()
        pltpu.make_async_copy(vt_ref.at[p], vt_ref.at[p], vt_recv.at[p]).wait()
        pltpu.make_async_copy(qk_ref.at[p], qk_in, in_sem.at[0]).start()
        pltpu.make_async_copy(vt_ref.at[p], vt_in, in_sem.at[1]).start()

    e = HEAD**-0.5 * LOG2E

    def attend(p):
        pltpu.make_async_copy(qk_ref.at[p], qk_in, in_sem.at[0]).wait()
        pltpu.make_async_copy(vt_ref.at[p], vt_in, in_sem.at[1]).wait()
        pieces = [(h, st) for h in range(PAIR) for st in range(2)]

        def queries(i, _):
            top_s[...] = jnp.full(top_s.shape, NEG, jnp.float32)
            mix_s[...] = jnp.zeros(mix_s.shape, jnp.float32)

            def block(j, diagonal):
                scores = []
                for h, st in pieces:
                    seen = half * (st + 1) if diagonal else own
                    keys = qk_in[K, h, pl.ds(pl.multiple_of(j * own, own), seen), :]
                    qs = qk_in[Q, h, pl.ds(pl.multiple_of(i * own + st * half, half), half), :]
                    scores.append(_dot(keys, qs, 1, 1))
                weights, keeps = [], []
                for c, ((h, st), s) in enumerate(zip(pieces, scores)):
                    if diagonal:
                        ok = lax.broadcasted_iota(jnp.int32, s.shape, 0) <= lax.broadcasted_iota(jnp.int32, s.shape, 1) + st * half
                        s = jnp.where(ok, s, HIDDEN)
                    old = top_s[c : c + 1, :]
                    top = jnp.maximum(old, s.max(axis=0, keepdims=True))
                    top_s[c : c + 1, :] = top
                    weights.append(jnp.exp2((s - top) * e).astype(jnp.bfloat16))
                    keeps.append(jnp.exp2((old - top) * e))
                for c, ((h, st), w, keep) in enumerate(zip(pieces, weights, keeps)):
                    seen = w.shape[0]
                    values = jnp.concatenate([vt_in[h, :, pl.ds(pl.multiple_of(j * own, own), seen)], jnp.ones((8, seen), jnp.bfloat16)], axis=0)
                    mix_s[c] = mix_s[c] * keep + _dot(values, w, 1, 0)
                return 0

            lax.fori_loop(0, i, lambda j, _: block(j, False), 0)
            block(i, True)

            away = i != me

            @pl.when(away & (p > 0))
            def _():
                pltpu.make_async_copy(o_out.at[i], o_out.at[i], o_send.at[i]).wait()

            for c, (h, st) in enumerate(pieces):
                total = mix_s[c, HEAD : HEAD + 1, :]
                o_out[i, st * half : (st + 1) * half, h * HEAD : (h + 1) * HEAD] = (mix_s[c, :HEAD, :] * (1 / total)).T.astype(jnp.bfloat16)
            place = pl.ds(pl.multiple_of(me * TILE, TILE), TILE)

            @pl.when(away)
            def _():
                pltpu.make_async_remote_copy(o_out.at[i], o_in.at[p, :, place], o_send.at[i], o_recv.at[p],
                                             device_id={"sp": i}, device_id_type=MESH).start()

            @pl.when(jnp.logical_not(away))
            def _():
                o_in[p, :, place] = o_out[i]
            return 0

        lax.fori_loop(0, n, queries, 0)

    def put(p):
        others = pl.ds(0, (n - 1) * TILE)
        pltpu.make_async_copy(o_in.at[p, :, others], o_in.at[p, :, others], o_recv.at[p]).wait()

        def step(part, _):
            s = proj_steps + p * n + part
            slot = weights_here(s)

            def one(c, _):
                cols = pl.ds(pl.multiple_of((part * per_step + c) * TILE, TILE), TILE)
                rows = pl.ds(pl.multiple_of(c * depth, depth), depth)
                total = acc[:, cols] + jnp.dot(o_in[p], wbuf[slot, rows, :], preferred_element_type=jnp.float32)
                acc[:, cols] = total

                @pl.when(p == pairs - 1)
                def _():
                    a[:, cols] = total.astype(jnp.bfloat16)
                return 0

            lax.fori_loop(0, per_step, one, 0)
            fetch(s + NW)

            @pl.when(p == pairs - 1)
            def _():
                cols = pl.ds(pl.multiple_of(part * per_step * TILE, TILE), per_step * TILE)
                pltpu.make_async_copy(a.at[:, cols], y_ref.at[:, cols], y_sem).start()
            return 0

        lax.fori_loop(0, n, step, 0)

    late = min(2, pairs)

    def turn(p, _):
        @pl.when(p < pairs)
        def _():
            lax.fori_loop(0, n_qk, lambda t, _: (project_qk(p, t), 0)[1], 0)

            def one(t, _):
                @pl.when((p > 0) & (t == tiles - 1))
                def _():
                    load_pair(p - 1)
                project_vt(p, t)
                return 0

            lax.fori_loop(n_qk, tiles, one, 0)

        first = jnp.where(p == pairs + 1, pairs - late, 0)
        last = jnp.where(p < pairs, 0, jnp.where(p == pairs, pairs - late, pairs))

        @pl.when(p == pairs)
        def _():
            load_pair(p - 1)

        lax.fori_loop(first, last, lambda k, _: (put(k), 0)[1], 0)

        @pl.when((p > 0) & (p <= pairs))
        def _():
            attend(p - 1)
        return 0

    lax.fori_loop(0, pairs + 2, turn, 0)

    pltpu.make_async_copy(a, y_ref, y_sem).wait()
    for slot in range(2 * n_qk):
        if slot % n != n - 1:
            pltpu.make_async_copy(qk_out.at[slot], qk_out.at[slot], qk_send.at[slot]).wait()
    for slot in range(2 * n_vt):
        if slot % n != n - 1:
            pltpu.make_async_copy(vt_out.at[slot], vt_out.at[slot], vt_send.at[slot]).wait()
    for i in range(n):
        @pl.when(i != me)
        def _():
            pltpu.make_async_copy(o_out.at[i], o_out.at[i], o_send.at[i]).wait()


def solution(mesh):
    n = mesh.shape["sp"]

    def step(x, gain, wq, wk, wv, wo):
        own, d = x.shape
        heads = wq.shape[1] // HEAD
        pairs = heads // n // PAIR
        seq = n * own
        place = lax.axis_index("sp") * own + jnp.arange(own)
        angle = place.astype(jnp.float32)[:, None] * THETA ** (-jnp.arange(HEAD // 2, dtype=jnp.float32) / (HEAD // 2))
        cos, sin = jnp.cos(angle), jnp.sin(angle)
        bf16, f32, dma = jnp.bfloat16, jnp.float32, pltpu.SemaphoreType.DMA
        vmem, hbm = pl.BlockSpec(memory_space=pltpu.VMEM), pl.BlockSpec(memory_space=pl.ANY)
        flops = 2 * own * d * 4 * heads * HEAD + 2 * heads // n * seq * seq * HEAD
        y, _, _ = pl.pallas_call(
            functools.partial(_kernel, n, pairs),
            out_shape=[jax.ShapeDtypeStruct((own, d), bf16), jax.ShapeDtypeStruct((pairs, 2, PAIR, seq, HEAD), bf16),
                       jax.ShapeDtypeStruct((pairs, PAIR, HEAD, seq), bf16)],
            in_specs=[hbm, vmem, vmem, vmem, hbm, hbm, hbm, hbm],
            out_specs=[hbm, hbm, hbm],
            scratch_shapes=[
                pltpu.VMEM((own, d), bf16),
                pltpu.VMEM((own, d), f32),
                pltpu.VMEM((NW, d, TILE), bf16),
                pltpu.VMEM((4 * n, PAIR, own, HEAD), bf16),
                pltpu.VMEM((2 * n, PAIR, HEAD, own), bf16),
                pltpu.VMEM((n, own, TILE), bf16),
                pltpu.VMEM((pairs, own, n * TILE), bf16),
                pltpu.VMEM((2, PAIR, seq, HEAD), bf16),
                pltpu.VMEM((PAIR, HEAD, seq), bf16),
                pltpu.VMEM((8, own // 2), f32),
                pltpu.VMEM((2 * PAIR, HEAD + 8, own // 2), f32),
                dma((NW,)), dma(()), dma(()), dma((2,)), dma((4 * n,)), dma((2 * n,)), dma((n,)), dma((pairs,)), dma((pairs,)), dma((pairs,)),
            ],
            compiler_params=pltpu.CompilerParams(collective_id=0, has_side_effects=True, vmem_limit_bytes=66 * 10**6),
            cost_estimate=pl.CostEstimate(flops=flops, transcendentals=heads // n * seq * seq // 2, bytes_accessed=2 * 4 * d * d),
            name="attention_half",
        )(x, gain.astype(f32)[None], jnp.concatenate([cos, cos], -1), jnp.concatenate([-sin, sin], -1), wq, wk, wv, wo)
        return y

    tokens, whole = P(("dp", "sp"), None), P(None, None)
    return jax.shard_map(step, mesh=mesh, in_specs=(tokens, P(None), whole, whole, whole, whole), out_specs=tokens, check_vma=False)
```

```python
import functools

import jax
import jax.numpy as jnp
from jax import lax
from jax.experimental import pallas as pl
from jax.experimental.pallas import tpu as pltpu
from jax.sharding import PartitionSpec as P

HEAD = 128
THETA = 10000
NEG = -1e30
HIDDEN = 2 * NEG
LOG2E = 1.4426950408889634
PAIR = 2
TILE = PAIR * HEAD
NW = 3
ROWS = 16
MESH = pl.DeviceIdType.MESH
Q, K = 0, 1


def _dot(a, b, ca, cb):
    return lax.dot_general(a, b, (((ca,), (cb,)), ((), ())), preferred_element_type=jnp.float32)


def _kernel(n, pairs, x_ref, gain_ref, cos_ref, sin_ref, wq, wk, wv, wo, y_ref, qk_ref, vt_ref,
            a, acc, wbuf, qk_out, vt_out, o_out, o_in, qk_in, vt_in, top_s, mix_s,
            w_sem, x_sem, y_sem, in_sem, qk_send, vt_send, o_send, qk_recv, vt_recv, o_recv):
    own, d = a.shape
    me = lax.axis_index("sp")
    wide = d // TILE
    per_step = wide // n
    depth = n * TILE
    n_qk, n_vt = 2 * n, n
    tiles = n_qk + n_vt
    proj_steps = pairs * tiles
    steps = proj_steps + pairs * n
    half = own // 2

    def column(owner, p):
        return pl.multiple_of((owner * pairs + p) * TILE, TILE)

    def owner_of(t):
        return lax.rem(me + lax.rem(t, n) + 1, n)

    def fetch(s):
        slot = lax.rem(s, NW)

        @pl.when(s < proj_steps)
        def _():
            p, t = lax.div(s, tiles), lax.rem(s, tiles)
            cols = pl.ds(column(owner_of(t), p), TILE)
            for i, w in enumerate((wq, wk, wv)):
                @pl.when(lax.div(t, n) == i)
                def _():
                    pltpu.make_async_copy(w.at[:, cols], wbuf.at[slot], w_sem.at[slot]).start()

        @pl.when((s >= proj_steps) & (s < steps))
        def _():
            p, part = lax.div(s - proj_steps, n), lax.rem(s - proj_steps, n)

            def one(c, _):
                cols = pl.ds(pl.multiple_of((part * per_step + c) * TILE, TILE), TILE)
                for owner in range(n):
                    pltpu.make_async_copy(wo.at[pl.ds(column(owner, p), TILE), cols],
                                          wbuf.at[slot, pl.ds(pl.multiple_of(c * depth + owner * TILE, TILE), TILE), :], w_sem.at[slot]).start()
                return 0

            lax.fori_loop(0, per_step, one, 0)

    def weights_here(s):
        slot = lax.rem(s, NW)
        pltpu.make_async_copy(wbuf.at[slot], wbuf.at[slot], w_sem.at[slot]).wait()
        return slot

    barrier = pltpu.get_barrier_semaphore()
    for r in range(1, n):
        pl.semaphore_signal(barrier, inc=1, device_id={"sp": lax.rem(me + r, n)}, device_id_type=MESH)
    pltpu.make_async_copy(x_ref, a, x_sem).start()
    for s in range(NW):
        fetch(jnp.int32(s))
    pltpu.make_async_copy(x_ref, a, x_sem).wait()

    def norm(i, _):
        rows = pl.ds(pl.multiple_of(i * ROWS, ROWS), ROWS)
        xr = a[rows, :].astype(jnp.float32)
        acc[rows, :] = xr
        scale = lax.rsqrt(jnp.mean(xr * xr, -1, keepdims=True) + 1e-6)
        a[rows, :] = (xr * scale * gain_ref[...]).astype(jnp.bfloat16)
        return 0

    lax.fori_loop(0, own // ROWS, norm, 0)
    pl.semaphore_wait(barrier, n - 1)

    def tile_of(s):
        slot = weights_here(s)
        t = jnp.dot(a[...], wbuf[slot], preferred_element_type=jnp.float32).astype(jnp.bfloat16)
        fetch(s + NW)
        return t

    mine = pl.ds(pl.multiple_of(me * own, own), own)

    def project_qk(p, t):
        tile = tile_of(p * tiles + t)
        m, owner, use = lax.div(t, n), owner_of(t), p * n_qk + t
        slot = lax.rem(use, 2 * n_qk)
        away = owner != me

        @pl.when(away & (use >= 2 * n_qk))
        def _():
            pltpu.make_async_copy(qk_out.at[slot], qk_out.at[slot], qk_send.at[slot]).wait()

        for h in range(PAIR):
            one = tile[:, h * HEAD : (h + 1) * HEAD].astype(jnp.float32)
            turned = one * cos_ref[...] + pltpu.roll(one, HEAD // 2, 1) * sin_ref[...]
            qk_out[slot, h] = turned.astype(jnp.bfloat16)

        @pl.when(away)
        def _():
            pltpu.make_async_remote_copy(qk_out.at[slot], qk_ref.at[p, m, :, mine, :], qk_send.at[slot], qk_recv.at[p],
                                         device_id={"sp": owner}, device_id_type=MESH).start()

        @pl.when(jnp.logical_not(away))
        def _():
            pltpu.make_async_copy(qk_out.at[slot], qk_ref.at[p, m, :, mine, :], qk_recv.at[p]).start()

    def project_vt(p, t):
        tile = tile_of(p * tiles + t)
        owner, use = owner_of(t), p * n_vt + t - n_qk
        slot = lax.rem(use, 2 * n_vt)
        away = owner != me

        @pl.when(away & (use >= 2 * n_vt))
        def _():
            pltpu.make_async_copy(vt_out.at[slot], vt_out.at[slot], vt_send.at[slot]).wait()

        for h in range(PAIR):
            vt_out[slot, h] = tile[:, h * HEAD : (h + 1) * HEAD].T

        @pl.when(away)
        def _():
            pltpu.make_async_remote_copy(vt_out.at[slot], vt_ref.at[p, :, :, mine], vt_send.at[slot], vt_recv.at[p],
                                         device_id={"sp": owner}, device_id_type=MESH).start()

        @pl.when(jnp.logical_not(away))
        def _():
            pltpu.make_async_copy(vt_out.at[slot], vt_ref.at[p, :, :, mine], vt_recv.at[p]).start()

    def load_pair(p):
        pltpu.make_async_copy(qk_ref.at[p], qk_ref.at[p], qk_recv.at[p]).wait()
        pltpu.make_async_copy(vt_ref.at[p], vt_ref.at[p], vt_recv.at[p]).wait()
        pltpu.make_async_copy(qk_ref.at[p], qk_in, in_sem.at[0]).start()
        pltpu.make_async_copy(vt_ref.at[p], vt_in, in_sem.at[1]).start()

    e = HEAD**-0.5 * LOG2E

    def attend(p):
        pltpu.make_async_copy(qk_ref.at[p], qk_in, in_sem.at[0]).wait()
        pltpu.make_async_copy(vt_ref.at[p], vt_in, in_sem.at[1]).wait()

        top_s[...] = jnp.full(top_s.shape, NEG, jnp.float32)
        mix_s[...] = jnp.zeros(mix_s.shape, jnp.float32)

        def block(*parts):
            pieces = [(i, j, diagonal, h, st) for i, j, diagonal in parts for h in range(PAIR) for st in range(2)]
            scores = []
            for i, j, diagonal, h, st in pieces:
                seen = half * (st + 1) if diagonal else own
                keys = qk_in[K, h, pl.ds(pl.multiple_of(j * own, own), seen), :]
                qs = qk_in[Q, h, i * own + st * half : i * own + (st + 1) * half, :]
                scores.append(_dot(keys, qs, 1, 1))
            weights, keeps = [], []
            for (i, j, diagonal, h, st), s in zip(pieces, scores):
                c = (i * PAIR + h) * 2 + st
                if diagonal:
                    ok = lax.broadcasted_iota(jnp.int32, s.shape, 0) <= lax.broadcasted_iota(jnp.int32, s.shape, 1) + st * half
                    s = jnp.where(ok, s, HIDDEN)
                old = top_s[c : c + 1, :]
                top = jnp.maximum(old, s.max(axis=0, keepdims=True))
                top_s[c : c + 1, :] = top
                weights.append(jnp.exp2((s - top) * e).astype(jnp.bfloat16))
                keeps.append(jnp.exp2((old - top) * e))
            for (i, j, diagonal, h, st), w, keep in zip(pieces, weights, keeps):
                c, seen = (i * PAIR + h) * 2 + st, w.shape[0]
                values = jnp.concatenate([vt_in[h, :, pl.ds(pl.multiple_of(j * own, own), seen)], jnp.ones((8, seen), jnp.bfloat16)], axis=0)
                mix_s[c] = mix_s[c] * keep + _dot(values, w, 1, 0)

        def finish(i):
            away = i != me

            @pl.when(away & (p > 0))
            def _():
                pltpu.make_async_copy(o_out.at[i], o_out.at[i], o_send.at[i]).wait()

            for h in range(PAIR):
                for st in range(2):
                    c = (i * PAIR + h) * 2 + st
                    total = mix_s[c, HEAD : HEAD + 1, :]
                    o_out[i, st * half : (st + 1) * half, h * HEAD : (h + 1) * HEAD] = (mix_s[c, :HEAD, :] * (1 / total)).T.astype(jnp.bfloat16)
            place = pl.ds(pl.multiple_of(me * TILE, TILE), TILE)

            @pl.when(away)
            def _():
                pltpu.make_async_remote_copy(o_out.at[i], o_in.at[p, :, place], o_send.at[i], o_recv.at[p],
                                             device_id={"sp": i}, device_id_type=MESH).start()

            @pl.when(jnp.logical_not(away))
            def _():
                o_in[p, :, place] = o_out[i]

        for hi in range(n - 1, 0, -2):
            lo = hi - 1
            if lo:
                lax.fori_loop(0, lo, lambda j, _: (block((hi, j, False), (lo, j, False)), 0)[1], 0)
            block((hi, lo, False), (lo, lo, True))
            finish(lo)
        if n % 2:
            block((0, 0, True))
            finish(0)
        last = list(range(n - 1, 0, -2))
        for at in range(0, len(last), 2):
            block(*((i, i, True) for i in last[at : at + 2]))
        for i in last:
            finish(i)

    def put(p):
        others = pl.ds(0, (n - 1) * TILE)
        pltpu.make_async_copy(o_in.at[p, :, others], o_in.at[p, :, others], o_recv.at[p]).wait()

        def step(part, _):
            s = proj_steps + p * n + part
            slot = weights_here(s)

            for c in range(per_step):
                cols = pl.ds(pl.multiple_of((part * per_step + c) * TILE, TILE), TILE)
                acc[:, cols] += jnp.dot(o_in[p], wbuf[slot, c * depth : (c + 1) * depth, :], preferred_element_type=jnp.float32)
            fetch(s + NW)

            @pl.when(p == pairs - 1)
            def _():
                cols = pl.ds(pl.multiple_of(part * per_step * TILE, TILE), per_step * TILE)
                a[:, cols] = acc[:, cols].astype(jnp.bfloat16)
                pltpu.make_async_copy(a.at[:, cols], y_ref.at[:, cols], y_sem).start()
            return 0

        lax.fori_loop(0, n, step, 0)

    late = min(2, pairs)

    def turn(p, _):
        @pl.when(p < pairs)
        def _():
            lax.fori_loop(0, n_qk, lambda t, _: (project_qk(p, t), 0)[1], 0)

            def one(t, _):
                @pl.when((p > 0) & (t == tiles - 1))
                def _():
                    load_pair(p - 1)
                project_vt(p, t)
                return 0

            lax.fori_loop(n_qk, tiles, one, 0)

        first = jnp.where(p == pairs + 1, pairs - late, 0)
        last = jnp.where(p < pairs, 0, jnp.where(p == pairs, pairs - late, pairs))

        @pl.when(p == pairs)
        def _():
            load_pair(p - 1)

        lax.fori_loop(first, last, lambda k, _: (put(k), 0)[1], 0)

        @pl.when((p > 0) & (p <= pairs))
        def _():
            attend(p - 1)
        return 0

    lax.fori_loop(0, pairs + 2, turn, 0)

    pltpu.make_async_copy(a, y_ref, y_sem).wait()
    for slot in range(2 * n_qk):
        if slot % n != n - 1:
            pltpu.make_async_copy(qk_out.at[slot], qk_out.at[slot], qk_send.at[slot]).wait()
    for slot in range(2 * n_vt):
        if slot % n != n - 1:
            pltpu.make_async_copy(vt_out.at[slot], vt_out.at[slot], vt_send.at[slot]).wait()
    for i in range(n):
        @pl.when(i != me)
        def _():
            pltpu.make_async_copy(o_out.at[i], o_out.at[i], o_send.at[i]).wait()


def solution(mesh):
    n = mesh.shape["sp"]

    def step(x, gain, wq, wk, wv, wo):
        own, d = x.shape
        heads = wq.shape[1] // HEAD
        pairs = heads // n // PAIR
        seq = n * own
        place = lax.axis_index("sp") * own + jnp.arange(own)
        angle = place.astype(jnp.float32)[:, None] * THETA ** (-jnp.arange(HEAD // 2, dtype=jnp.float32) / (HEAD // 2))
        cos, sin = jnp.cos(angle), jnp.sin(angle)
        bf16, f32, dma = jnp.bfloat16, jnp.float32, pltpu.SemaphoreType.DMA
        vmem, hbm = pl.BlockSpec(memory_space=pltpu.VMEM), pl.BlockSpec(memory_space=pl.ANY)
        flops = 2 * own * d * 4 * heads * HEAD + 2 * heads // n * seq * seq * HEAD
        y, _, _ = pl.pallas_call(
            functools.partial(_kernel, n, pairs),
            out_shape=[jax.ShapeDtypeStruct((own, d), bf16), jax.ShapeDtypeStruct((pairs, 2, PAIR, seq, HEAD), bf16),
                       jax.ShapeDtypeStruct((pairs, PAIR, HEAD, seq), bf16)],
            in_specs=[hbm, vmem, vmem, vmem, hbm, hbm, hbm, hbm],
            out_specs=[hbm, hbm, hbm],
            scratch_shapes=[
                pltpu.VMEM((own, d), bf16),
                pltpu.VMEM((own, d), f32),
                pltpu.VMEM((NW, d, TILE), bf16),
                pltpu.VMEM((4 * n, PAIR, own, HEAD), bf16),
                pltpu.VMEM((2 * n, PAIR, HEAD, own), bf16),
                pltpu.VMEM((n, own, TILE), bf16),
                pltpu.VMEM((pairs, own, n * TILE), bf16),
                pltpu.VMEM((2, PAIR, seq, HEAD), bf16),
                pltpu.VMEM((PAIR, HEAD, seq), bf16),
                pltpu.VMEM((2 * n * PAIR, own // 2), f32),
                pltpu.VMEM((2 * n * PAIR, HEAD + 8, own // 2), f32),
                dma((NW,)), dma(()), dma(()), dma((2,)), dma((4 * n,)), dma((2 * n,)), dma((n,)), dma((pairs,)), dma((pairs,)), dma((pairs,)),
            ],
            compiler_params=pltpu.CompilerParams(collective_id=0, has_side_effects=True, vmem_limit_bytes=66 * 10**6),
            cost_estimate=pl.CostEstimate(flops=flops, transcendentals=heads // n * seq * seq // 2, bytes_accessed=2 * 4 * d * d),
            name="attention_half",
        )(x, gain.astype(f32)[None], jnp.concatenate([cos, cos], -1), jnp.concatenate([-sin, sin], -1), wq, wk, wv, wo)
        return y

    tokens, whole = P(("dp", "sp"), None), P(None, None)
    return jax.shard_map(step, mesh=mesh, in_specs=(tokens, P(None), whole, whole, whole, whole), out_specs=tokens, check_vma=False)
```

```python
import functools

import jax
import jax.numpy as jnp
from jax import lax
from jax.experimental import pallas as pl
from jax.experimental.pallas import tpu as pltpu
from jax.sharding import PartitionSpec as P

HEAD = 128
THETA = 10000
NEG = -1e30
HIDDEN = 2 * NEG
LOG2E = 1.4426950408889634
PAIR = 2
TILE = PAIR * HEAD
NW = 3
ROWS = 16
MESH = pl.DeviceIdType.MESH
Q, K = 0, 1
RELIEF = 1


def _dot(a, b, ca, cb):
    return lax.dot_general(a, b, (((ca,), (cb,)), ((), ())), preferred_element_type=jnp.float32)


def _kernel(n, pairs, x_ref, gain_ref, cos_ref, sin_ref, wq, wk, wv, wo, y_ref, qk_ref, vt_ref,
            a, acc, wbuf, qk_out, vt_out, o_out, o_in, qk_in, vt_in, top_s, mix_s, st_out, st_in, edge_top, edge_mix,
            w_sem, x_sem, y_sem, in_sem, qk_send, vt_send, o_send, st_send, q_recv, k_recv, vt_recv, o_recv, st_recv):
    own, d = a.shape
    me = lax.axis_index("sp")
    wide = d // TILE
    per_step = wide // n
    depth = n * TILE
    n_qk, n_vt = 2 * n, n
    tiles = n_qk + n_vt
    proj_steps = pairs * tiles
    steps = proj_steps + pairs * n
    half = own // 2
    first_one, last_one = me == 0, me == n - 1

    def column(owner, p):
        return pl.multiple_of((owner * pairs + p) * TILE, TILE)

    def owner_of(t):
        return lax.rem(me + lax.rem(t, n) + 1, n)

    def fetch(s):
        slot = lax.rem(s, NW)

        @pl.when(s < proj_steps)
        def _():
            p, t = lax.div(s, tiles), lax.rem(s, tiles)
            cols = pl.ds(column(owner_of(t), p), TILE)
            for i, w in enumerate((wq, wk, wv)):
                @pl.when(lax.div(t, n) == i)
                def _():
                    pltpu.make_async_copy(w.at[:, cols], wbuf.at[slot], w_sem.at[slot]).start()

        @pl.when((s >= proj_steps) & (s < steps))
        def _():
            p, part = lax.div(s - proj_steps, n), lax.rem(s - proj_steps, n)

            def one(c, _):
                cols = pl.ds(pl.multiple_of((part * per_step + c) * TILE, TILE), TILE)
                for owner in range(n):
                    pltpu.make_async_copy(wo.at[pl.ds(column(owner, p), TILE), cols],
                                          wbuf.at[slot, pl.ds(pl.multiple_of(c * depth + owner * TILE, TILE), TILE), :], w_sem.at[slot]).start()
                return 0

            lax.fori_loop(0, per_step, one, 0)

    def weights_here(s):
        slot = lax.rem(s, NW)
        pltpu.make_async_copy(wbuf.at[slot], wbuf.at[slot], w_sem.at[slot]).wait()
        return slot

    barrier = pltpu.get_barrier_semaphore()
    for r in range(1, n):
        pl.semaphore_signal(barrier, inc=1, device_id={"sp": lax.rem(me + r, n)}, device_id_type=MESH)
    pltpu.make_async_copy(x_ref, a, x_sem).start()
    for s in range(NW):
        fetch(jnp.int32(s))
    pltpu.make_async_copy(x_ref, a, x_sem).wait()

    def norm(i, _):
        rows = pl.ds(pl.multiple_of(i * ROWS, ROWS), ROWS)
        xr = a[rows, :].astype(jnp.float32)
        acc[rows, :] = xr
        scale = lax.rsqrt(jnp.mean(xr * xr, -1, keepdims=True) + 1e-6)
        a[rows, :] = (xr * scale * gain_ref[...]).astype(jnp.bfloat16)
        return 0

    lax.fori_loop(0, own // ROWS, norm, 0)
    pl.semaphore_wait(barrier, n - 1)

    def tile_of(s):
        slot = weights_here(s)
        t = jnp.dot(a[...], wbuf[slot], preferred_element_type=jnp.float32).astype(jnp.bfloat16)
        fetch(s + NW)
        return t

    mine = pl.ds(pl.multiple_of(me * own, own), own)

    def stays_here(m, owner):
        return (first_one & (m == Q)) | (last_one & (m != Q) & (owner == RELIEF))

    def project_qk(p, t):
        tile = tile_of(p * tiles + t)
        m, owner, use = lax.div(t, n), owner_of(t), p * n_qk + t
        slot = lax.rem(use, 2 * n_qk)
        stays = stays_here(m, owner)
        away = (owner != me) & jnp.logical_not(stays)

        @pl.when(away & (use >= 2 * n_qk))
        def _():
            pltpu.make_async_copy(qk_out.at[slot], qk_out.at[slot], qk_send.at[slot]).wait()

        for h in range(PAIR):
            one = tile[:, h * HEAD : (h + 1) * HEAD].astype(jnp.float32)
            turned = one * cos_ref[...] + pltpu.roll(one, HEAD // 2, 1) * sin_ref[...]
            qk_out[slot, h] = turned.astype(jnp.bfloat16)

        for kind, recv in ((Q, q_recv), (K, k_recv)):
            @pl.when(away & (m == kind))
            def _():
                pltpu.make_async_remote_copy(qk_out.at[slot], qk_ref.at[p, kind, :, mine, :], qk_send.at[slot], recv.at[p],
                                             device_id={"sp": owner}, device_id_type=MESH).start()

            @pl.when((owner == me) & jnp.logical_not(stays) & (m == kind))
            def _():
                pltpu.make_async_copy(qk_out.at[slot], qk_ref.at[p, kind, :, mine, :], recv.at[p]).start()

    def project_vt(p, t):
        tile = tile_of(p * tiles + t)
        owner, use = owner_of(t), p * n_vt + t - n_qk
        slot = lax.rem(use, 2 * n_vt)
        away = (owner != me) & jnp.logical_not(stays_here(2, owner))

        @pl.when(away & (use >= 2 * n_vt))
        def _():
            pltpu.make_async_copy(vt_out.at[slot], vt_out.at[slot], vt_send.at[slot]).wait()

        for h in range(PAIR):
            vt_out[slot, h] = tile[:, h * HEAD : (h + 1) * HEAD].T

        @pl.when(away)
        def _():
            pltpu.make_async_remote_copy(vt_out.at[slot], vt_ref.at[p, :, :, mine], vt_send.at[slot], vt_recv.at[p],
                                         device_id={"sp": owner}, device_id_type=MESH).start()

        @pl.when(owner == me)
        def _():
            pltpu.make_async_copy(vt_out.at[slot], vt_ref.at[p, :, :, mine], vt_recv.at[p]).start()

    def load_pair(p):
        here = qk_ref.at[p, Q, :, pl.ds(own, (n - 1) * own), :]
        pltpu.make_async_copy(here, here, q_recv.at[p]).wait()
        for relieved, blocks in ((True, n - 1), (False, n)):
            @pl.when((me == RELIEF) == relieved)
            def _():
                keys, values = qk_ref.at[p, K, :, pl.ds(0, blocks * own), :], vt_ref.at[p, :, :, pl.ds(0, blocks * own)]
                pltpu.make_async_copy(keys, keys, k_recv.at[p]).wait()
                pltpu.make_async_copy(values, values, vt_recv.at[p]).wait()
        pltpu.make_async_copy(qk_ref.at[p], qk_in, in_sem.at[0]).start()
        pltpu.make_async_copy(vt_ref.at[p], vt_in, in_sem.at[1]).start()

    e = HEAD**-0.5 * LOG2E

    def attend(p):
        pltpu.make_async_copy(qk_ref.at[p], qk_in, in_sem.at[0]).wait()
        pltpu.make_async_copy(vt_ref.at[p], vt_in, in_sem.at[1]).wait()

        top_s[...] = jnp.full(top_s.shape, NEG, jnp.float32)
        mix_s[...] = jnp.zeros(mix_s.shape, jnp.float32)

        def block(*parts):
            pieces = [(i, j, diagonal, h, st) for i, j, diagonal in parts for h in range(PAIR) for st in range(2)]
            scores = []
            for i, j, diagonal, h, st in pieces:
                seen = half * (st + 1) if diagonal else own
                keys = qk_in[K, h, pl.ds(pl.multiple_of(j * own, own), seen), :]
                qs = qk_in[Q, h, i * own + st * half : i * own + (st + 1) * half, :]
                scores.append(_dot(keys, qs, 1, 1))
            weights, keeps = [], []
            for (i, j, diagonal, h, st), s in zip(pieces, scores):
                c = (i * PAIR + h) * 2 + st
                if diagonal:
                    ok = lax.broadcasted_iota(jnp.int32, s.shape, 0) <= lax.broadcasted_iota(jnp.int32, s.shape, 1) + st * half
                    s = jnp.where(ok, s, HIDDEN)
                old = top_s[c : c + 1, :]
                top = jnp.maximum(old, s.max(axis=0, keepdims=True))
                top_s[c : c + 1, :] = top
                weights.append(jnp.exp2((s - top) * e).astype(jnp.bfloat16))
                keeps.append(jnp.exp2((old - top) * e))
            for (i, j, diagonal, h, st), w, keep in zip(pieces, weights, keeps):
                c, seen = (i * PAIR + h) * 2 + st, w.shape[0]
                values = jnp.concatenate([vt_in[h, :, pl.ds(pl.multiple_of(j * own, own), seen)], jnp.ones((8, seen), jnp.bfloat16)], axis=0)
                mix_s[c] = mix_s[c] * keep + _dot(values, w, 1, 0)

        def finish(i):
            away = i != me

            @pl.when(away & (p > 0))
            def _():
                pltpu.make_async_copy(o_out.at[i], o_out.at[i], o_send.at[i]).wait()

            for h in range(PAIR):
                for st in range(2):
                    c = (i * PAIR + h) * 2 + st
                    total = mix_s[c, HEAD : HEAD + 1, :]
                    o_out[i, st * half : (st + 1) * half, h * HEAD : (h + 1) * HEAD] = (mix_s[c, :HEAD, :] * (1 / total)).T.astype(jnp.bfloat16)
            place = pl.ds(pl.multiple_of(me * TILE, TILE), TILE)

            @pl.when(away)
            def _():
                pltpu.make_async_remote_copy(o_out.at[i], o_in.at[p, :, place], o_send.at[i], o_recv.at[p],
                                             device_id={"sp": i}, device_id_type=MESH).start()

            @pl.when(jnp.logical_not(away))
            def _():
                o_in[p, :, place] = o_out[i]

        top_block = n - 1
        for hi in range(top_block, 1, -2):
            lo = hi - 1
            lax.fori_loop(0, lo, lambda j, _: (block((hi, j, False), (lo, j, False)), 0)[1], 0)
            block((hi, lo, False), (lo, lo, True))
            finish(lo)
            if hi != top_block:
                block((hi, hi, True))
                finish(hi)
        if n % 2 == 0:
            block((1, 0, False), (1, 1, True))
            finish(1)

        @pl.when(me != RELIEF)
        def _():
            block((top_block, top_block, True))

        @pl.when(me == RELIEF)
        def _():
            @pl.when(p > 0)
            def _():
                pltpu.make_async_copy(st_out, st_out, st_send).wait()

            for h in range(PAIR):
                for st in range(2):
                    c = (top_block * PAIR + h) * 2 + st
                    st_out[2 * h : 2 * h + 1, st * half : (st + 1) * half] = top_s[c : c + 1, :]
                    st_out[2 * h + 1 : 2 * h + 2, st * half : (st + 1) * half] = mix_s[c, HEAD : HEAD + 1, :]
            pltpu.make_async_remote_copy(st_out, st_in.at[p], st_send, st_recv.at[p], device_id={"sp": top_block}, device_id_type=MESH).start()

        finish(top_block)

    def corner(p, owners):
        pieces, scores, found = [], [], []
        for owner in owners:
            t = lax.rem(owner - me - 1 + n, n)
            q_at, k_at, v_at = lax.rem(p * n_qk + t, 2 * n_qk), lax.rem(p * n_qk + n + t, 2 * n_qk), lax.rem(p * n_vt + t, 2 * n_vt)
            for h in range(PAIR):
                for st in range(2):
                    pieces.append((owner, v_at, h, st))
                    scores.append(_dot(qk_out[k_at, h, : half * (st + 1), :], qk_out[q_at, h, st * half : (st + 1) * half, :], 1, 1))
        weights = []
        for (owner, v_at, h, st), s in zip(pieces, scores):
            ok = lax.broadcasted_iota(jnp.int32, s.shape, 0) <= lax.broadcasted_iota(jnp.int32, s.shape, 1) + st * half
            s = jnp.where(ok, s, HIDDEN)
            top = s.max(axis=0, keepdims=True)
            weights.append((top, jnp.exp2((s - top) * e).astype(jnp.bfloat16)))
        for (owner, v_at, h, st), (top, w) in zip(pieces, weights):
            seen = w.shape[0]
            values = jnp.concatenate([vt_out[v_at, h, :, :seen], jnp.ones((8, seen), jnp.bfloat16)], axis=0)
            found.append((owner, h, st, top, _dot(values, w, 1, 0)))
        return found

    def corners(p):
        @pl.when(first_one)
        def _():
            def some(k, _):
                for owner, h, st, _top, mix in corner(p, [2 * k, 2 * k + 1]):
                    lanes = pl.ds(pl.multiple_of(owner * TILE + h * HEAD, HEAD), HEAD)
                    o_in[p, st * half : (st + 1) * half, lanes] = (mix[:HEAD] * (1 / mix[HEAD : HEAD + 1])).T.astype(jnp.bfloat16)
                return 0

            lax.fori_loop(0, n // 2, some, 0)

        @pl.when(last_one)
        def _():
            for owner, h, st, top, mix in corner(p, [RELIEF]):
                edge_top[p, h * 2 + st : h * 2 + st + 1, :] = top
                edge_mix[p, h * 2 + st] = mix

    def join(p):
        pltpu.make_async_copy(st_in.at[p], st_in.at[p], st_recv.at[p]).wait()
        for h in range(PAIR):
            for st in range(2):
                rows, lanes = slice(st * half, (st + 1) * half), slice(RELIEF * TILE + h * HEAD, RELIEF * TILE + (h + 1) * HEAD)
                c = h * 2 + st
                far_top, far_total = st_in[p, 2 * h : 2 * h + 1, rows], st_in[p, 2 * h + 1 : 2 * h + 2, rows]
                near_top, near = edge_top[p, c : c + 1, :], edge_mix[p, c]
                top = jnp.maximum(far_top, near_top)
                far_w, near_w = far_total * jnp.exp2((far_top - top) * e), jnp.exp2((near_top - top) * e)
                far = o_in[p, rows, lanes].astype(jnp.float32).T
                out = (far * far_w + near[:HEAD] * near_w) * (1 / (far_w + near[HEAD : HEAD + 1] * near_w))
                o_in[p, rows, lanes] = out.T.astype(jnp.bfloat16)

    def put(p):
        others = pl.ds(0, (n - 1) * TILE)

        @pl.when(jnp.logical_not(first_one))
        def _():
            pltpu.make_async_copy(o_in.at[p, :, others], o_in.at[p, :, others], o_recv.at[p]).wait()

        @pl.when(last_one)
        def _():
            join(p)

        def step(part, _):
            s = proj_steps + p * n + part
            slot = weights_here(s)

            for c in range(per_step):
                cols = pl.ds(pl.multiple_of((part * per_step + c) * TILE, TILE), TILE)
                acc[:, cols] += jnp.dot(o_in[p], wbuf[slot, c * depth : (c + 1) * depth, :], preferred_element_type=jnp.float32)
            fetch(s + NW)

            @pl.when(p == pairs - 1)
            def _():
                cols = pl.ds(pl.multiple_of(part * per_step * TILE, TILE), per_step * TILE)
                a[:, cols] = acc[:, cols].astype(jnp.bfloat16)
                pltpu.make_async_copy(a.at[:, cols], y_ref.at[:, cols], y_sem).start()
            return 0

        lax.fori_loop(0, n, step, 0)

    late = min(3, pairs)

    def turn(p, _):
        @pl.when(p < pairs)
        def _():
            lax.fori_loop(0, n_qk, lambda t, _: (project_qk(p, t), 0)[1], 0)

            def one(t, _):
                @pl.when((p > 0) & (t == tiles - 1))
                def _():
                    load_pair(p - 1)
                project_vt(p, t)
                return 0

            lax.fori_loop(n_qk, tiles, one, 0)
            corners(p)

        first = jnp.where(p == pairs + 1, pairs - late, 0)
        last = jnp.where(p < pairs, 0, jnp.where(p == pairs, pairs - late, pairs))

        lax.fori_loop(first, last, lambda k, _: (put(k), 0)[1], 0)

        @pl.when(p == pairs)
        def _():
            load_pair(p - 1)

        @pl.when((p > 0) & (p <= pairs))
        def _():
            attend(p - 1)
        return 0

    lax.fori_loop(0, pairs + 2, turn, 0)

    pltpu.make_async_copy(a, y_ref, y_sem).wait()
    for slot in range(2 * n_qk):
        if slot % n != n - 1:
            @pl.when(jnp.logical_not(stays_here(slot % n_qk // n, owner_of(slot))))
            def _():
                pltpu.make_async_copy(qk_out.at[slot], qk_out.at[slot], qk_send.at[slot]).wait()
    for slot in range(2 * n_vt):
        if slot % n != n - 1:
            @pl.when(jnp.logical_not(stays_here(2, owner_of(slot))))
            def _():
                pltpu.make_async_copy(vt_out.at[slot], vt_out.at[slot], vt_send.at[slot]).wait()

    @pl.when(me == RELIEF)
    def _():
        pltpu.make_async_copy(st_out, st_out, st_send).wait()

    for i in range(1, n):
        @pl.when(i != me)
        def _():
            pltpu.make_async_copy(o_out.at[i], o_out.at[i], o_send.at[i]).wait()


def solution(mesh):
    n = mesh.shape["sp"]

    def step(x, gain, wq, wk, wv, wo):
        own, d = x.shape
        heads = wq.shape[1] // HEAD
        pairs = heads // n // PAIR
        seq = n * own
        place = lax.axis_index("sp") * own + jnp.arange(own)
        angle = place.astype(jnp.float32)[:, None] * THETA ** (-jnp.arange(HEAD // 2, dtype=jnp.float32) / (HEAD // 2))
        cos, sin = jnp.cos(angle), jnp.sin(angle)
        bf16, f32, dma = jnp.bfloat16, jnp.float32, pltpu.SemaphoreType.DMA
        vmem, hbm = pl.BlockSpec(memory_space=pltpu.VMEM), pl.BlockSpec(memory_space=pl.ANY)
        flops = 2 * own * d * 4 * heads * HEAD + 2 * heads // n * seq * seq * HEAD
        y, _, _ = pl.pallas_call(
            functools.partial(_kernel, n, pairs),
            out_shape=[jax.ShapeDtypeStruct((own, d), bf16), jax.ShapeDtypeStruct((pairs, 2, PAIR, seq, HEAD), bf16),
                       jax.ShapeDtypeStruct((pairs, PAIR, HEAD, seq), bf16)],
            in_specs=[hbm, vmem, vmem, vmem, hbm, hbm, hbm, hbm],
            out_specs=[hbm, hbm, hbm],
            scratch_shapes=[
                pltpu.VMEM((own, d), bf16),
                pltpu.VMEM((own, d), f32),
                pltpu.VMEM((NW, d, TILE), bf16),
                pltpu.VMEM((4 * n, PAIR, own, HEAD), bf16),
                pltpu.VMEM((2 * n, PAIR, HEAD, own), bf16),
                pltpu.VMEM((n, own, TILE), bf16),
                pltpu.VMEM((pairs, own, n * TILE), bf16),
                pltpu.VMEM((2, PAIR, seq, HEAD), bf16),
                pltpu.VMEM((PAIR, HEAD, seq), bf16),
                pltpu.VMEM((2 * n * PAIR, own // 2), f32),
                pltpu.VMEM((2 * n * PAIR, HEAD + 8, own // 2), f32),
                pltpu.VMEM((8, own), f32),
                pltpu.VMEM((pairs, 8, own), f32),
                pltpu.VMEM((pairs, 8, own // 2), f32),
                pltpu.VMEM((pairs, 2 * PAIR, HEAD + 8, own // 2), f32),
                dma((NW,)), dma(()), dma(()), dma((2,)), dma((4 * n,)), dma((2 * n,)), dma((n,)), dma(()), dma((pairs,)), dma((pairs,)), dma((pairs,)),
                dma((pairs,)), dma((pairs,)),
            ],
            compiler_params=pltpu.CompilerParams(collective_id=0, has_side_effects=True, vmem_limit_bytes=66 * 10**6),
            cost_estimate=pl.CostEstimate(flops=flops, transcendentals=heads // n * seq * seq // 2, bytes_accessed=2 * 4 * d * d),
            name="attention_half",
        )(x, gain.astype(f32)[None], jnp.concatenate([cos, cos], -1), jnp.concatenate([-sin, sin], -1), wq, wk, wv, wo)
        return y

    tokens, whole = P(("dp", "sp"), None), P(None, None)
    return jax.shard_map(step, mesh=mesh, in_specs=(tokens, P(None), whole, whole, whole, whole), out_specs=tokens, check_vma=False)
```

```python
import functools

import jax
import jax.numpy as jnp
from jax import lax
from jax.experimental import pallas as pl
from jax.experimental.pallas import tpu as pltpu
from jax.sharding import PartitionSpec as P

HEAD = 128
THETA = 10000
NEG = -1e30
HIDDEN = 2 * NEG
LOG2E = 1.4426950408889634
PAIR = 2
TILE = PAIR * HEAD
NW = 3
ROWS = 16
MESH = pl.DeviceIdType.MESH
K, Q = 0, 1
RELIEF = 1


def _dot(a, b, ca, cb):
    return lax.dot_general(a, b, (((ca,), (cb,)), ((), ())), preferred_element_type=jnp.float32)


def _kernel(n, pairs, x_ref, gain_ref, cos_in, sin_in, wq, wk, wv, wo, y_ref, qk_ref, vt_ref,
            a, acc, wbuf, qk_out, vt_out, o_out, o_in, qk_in, vt_in, raw, cos_ref, sin_ref, top_s, mix_s, st_out, st_in, edge_top, edge_mix,
            w_sem, x_sem, y_sem, in_sem, qk_send, vt_send, o_send, st_send, q_recv, k_recv, vt_recv, o_recv, st_recv):
    own, d = a.shape
    me = lax.axis_index("sp")
    wide = d // TILE
    per_step = wide // n
    depth = n * TILE
    n_qk, n_vt = 2 * n, n
    tiles = n_qk + n_vt
    proj_steps = pairs * tiles
    steps = proj_steps + pairs * n
    half = own // 2
    first_one, last_one = me == 0, me == n - 1

    def column(owner, p):
        return pl.multiple_of((owner * pairs + p) * TILE, TILE)

    def owner_of(t):
        return lax.rem(me + lax.rem(t + n, n) + 1, n)

    def fetch(s):
        slot = lax.rem(s, NW)

        @pl.when(s < proj_steps)
        def _():
            p, t = lax.div(s, tiles), lax.rem(s, tiles)
            cols = pl.ds(column(owner_of(t), p), TILE)
            for i, w in enumerate((wk, wq, wv)):
                @pl.when(lax.div(t, n) == i)
                def _():
                    pltpu.make_async_copy(w.at[:, :, cols], wbuf.at[slot], w_sem.at[slot]).start(priority=1)

        @pl.when((s >= proj_steps) & (s < steps))
        def _():
            p, part = lax.div(s - proj_steps, n), lax.rem(s - proj_steps, n)

            for c in range(per_step):
                cols = pl.ds(pl.multiple_of((part * per_step + c) * TILE, TILE), TILE)
                pltpu.make_async_copy(wo.at[:, p, :, cols], wbuf.at[slot, c * n : (c + 1) * n], w_sem.at[slot]).start(priority=1)

    def weights_here(s):
        slot = lax.rem(s, NW)
        pltpu.make_async_copy(wbuf.at[slot], wbuf.at[slot], w_sem.at[slot]).wait()
        return slot

    barrier = pltpu.get_barrier_semaphore()
    for r in range(1, n):
        pl.semaphore_signal(barrier, inc=1, device_id={"sp": lax.rem(me + r, n)}, device_id_type=MESH)
    pltpu.make_async_copy(x_ref, a, x_sem).start()
    for s in range(NW):
        fetch(jnp.int32(s))
    pltpu.make_async_copy(x_ref, a, x_sem).wait()

    def norm(i, _):
        rows = pl.ds(pl.multiple_of(i * ROWS, ROWS), ROWS)
        xr = a[rows, :].astype(jnp.float32)
        acc[rows, :] = xr
        scale = lax.rsqrt(jnp.mean(xr * xr, -1, keepdims=True) + 1e-6)
        a[rows, :] = (xr * scale * gain_ref[...].astype(jnp.float32)).astype(jnp.bfloat16)
        return 0

    lax.fori_loop(0, own // ROWS, norm, 0, unroll=2)
    raw[...] = jnp.zeros_like(raw)
    cos_ref[...] = jnp.concatenate([cos_in[...], cos_in[...]], -1)
    sin_ref[...] = jnp.concatenate([-sin_in[...], sin_in[...]], -1)
    pl.semaphore_wait(barrier, n - 1)

    def next_tile(s):
        raw[...] = jnp.dot(a[...], wbuf[lax.rem(s, NW)].reshape(d, TILE), preferred_element_type=jnp.float32).astype(jnp.bfloat16)

    mine = pl.ds(pl.multiple_of(me * own, own), own)

    def stays_here(m, owner):
        return (first_one & (m == Q)) | (last_one & (m != Q) & (owner == RELIEF))

    def free(out, sent, slot, use, away):
        @pl.when(away & (use >= out.shape[0] - 1))
        def _():
            pltpu.make_async_copy(out.at[slot], out.at[slot], sent.at[slot]).wait()

    def project_qk(p, t, flush=False):
        before = t - 1
        m, owner, use = lax.div(before, n), owner_of(before), p * n_qk + before
        real = t > 0
        stays = stays_here(m, owner)
        away = real & (owner != me) & jnp.logical_not(stays)
        kept = real & (owner == me) & jnp.logical_not(stays)
        slot = jnp.where(real, lax.rem(use, 2 * n_qk), 2 * n_qk)
        free(qk_out, qk_send, slot, use, away)
        s = p * tiles + t
        if not flush:
            weights_here(s)
        for h in range(PAIR):
            one = raw[:, h * HEAD : (h + 1) * HEAD].astype(jnp.float32)
            turned = one * cos_ref[...] + pltpu.roll(one, HEAD // 2, 1) * sin_ref[...]
            qk_out[slot, h] = turned.astype(jnp.bfloat16)
        if not flush:
            next_tile(s)
            fetch(s + NW)
        for kind, recv in ((Q, q_recv), (K, k_recv)):
            @pl.when(away & (m == kind))
            def _():
                pltpu.make_async_remote_copy(qk_out.at[slot], qk_ref.at[p, kind, :, mine, :], qk_send.at[slot], recv.at[p],
                                             device_id={"sp": owner}, device_id_type=MESH).start()

            @pl.when(kept & (m == kind))
            def _():
                pltpu.make_async_copy(qk_out.at[slot], qk_ref.at[p, kind, :, mine, :], recv.at[p]).start()

    def project_vt(p, t, flush=False):
        before = t - 1
        owner, use = owner_of(before), p * n_vt + before - n_qk
        real = t > n_qk
        away = real & (owner != me) & jnp.logical_not(stays_here(2, owner))
        slot = jnp.where(real, lax.rem(use, 2 * n_vt), 2 * n_vt)
        free(vt_out, vt_send, slot, use, away)
        s = p * tiles + t
        if not flush:
            weights_here(s)
        for h in range(PAIR):
            vt_out[slot, h] = raw[:, h * HEAD : (h + 1) * HEAD].T
        if not flush:
            next_tile(s)
            fetch(s + NW)

        @pl.when(away)
        def _():
            pltpu.make_async_remote_copy(vt_out.at[slot], vt_ref.at[p, :, :, mine], vt_send.at[slot], vt_recv.at[p],
                                         device_id={"sp": owner}, device_id_type=MESH).start()

        @pl.when(real & (owner == me))
        def _():
            pltpu.make_async_copy(vt_out.at[slot], vt_ref.at[p, :, :, mine], vt_recv.at[p]).start()

    def load_pair(p):
        here = qk_ref.at[p, Q, :, pl.ds(own, (n - 1) * own), :]
        pltpu.make_async_copy(here, here, q_recv.at[p]).wait()
        for relieved, blocks in ((True, n - 1), (False, n)):
            @pl.when((me == RELIEF) == relieved)
            def _():
                keys, values = qk_ref.at[p, K, :, pl.ds(0, blocks * own), :], vt_ref.at[p, :, :, pl.ds(0, blocks * own)]
                pltpu.make_async_copy(keys, keys, k_recv.at[p]).wait()
                pltpu.make_async_copy(values, values, vt_recv.at[p]).wait()
        pltpu.make_async_copy(qk_ref.at[p], qk_in, in_sem.at[0]).start()
        pltpu.make_async_copy(vt_ref.at[p], vt_in, in_sem.at[1]).start()

    e = HEAD**-0.5 * LOG2E

    def attend(p):
        pltpu.make_async_copy(qk_ref.at[p], qk_in, in_sem.at[0]).wait()
        pltpu.make_async_copy(vt_ref.at[p], vt_in, in_sem.at[1]).wait()

        top_s[...] = jnp.full(top_s.shape, NEG, jnp.float32)
        mix_s[...] = jnp.zeros(mix_s.shape, jnp.float32)

        def block(*parts):
            pieces = [(i, j, diagonal, h, st) for i, j, diagonal in parts for h in range(PAIR) for st in range(2)]
            scores = []
            for i, j, diagonal, h, st in pieces:
                seen = half * (st + 1) if diagonal else own
                keys = qk_in[K, h, pl.ds(pl.multiple_of(j * own, own), seen), :]
                qs = qk_in[Q, h, i * own + st * half : i * own + (st + 1) * half, :]
                scores.append(_dot(keys, qs, 1, 1))
            weights, keeps = [], []
            for (i, j, diagonal, h, st), s in zip(pieces, scores):
                c = (i * PAIR + h) * 2 + st
                if diagonal:
                    ok = lax.broadcasted_iota(jnp.int32, s.shape, 0) <= lax.broadcasted_iota(jnp.int32, s.shape, 1) + st * half
                    s = jnp.where(ok, s, HIDDEN)
                old = top_s[c : c + 1, :]
                top = jnp.maximum(old, s.max(axis=0, keepdims=True))
                top_s[c : c + 1, :] = top
                weights.append(jnp.exp2((s - top) * e).astype(jnp.bfloat16))
                keeps.append(jnp.exp2((old - top) * e))
            for (i, j, diagonal, h, st), w, keep in zip(pieces, weights, keeps):
                c, seen = (i * PAIR + h) * 2 + st, w.shape[0]
                values = jnp.concatenate([vt_in[h, :, pl.ds(pl.multiple_of(j * own, own), seen)], jnp.ones((8, seen), jnp.bfloat16)], axis=0)
                mix_s[c] = mix_s[c] * keep + _dot(values, w, 1, 0)

        def finish(i):
            away = i != me

            @pl.when(away & (p > 0))
            def _():
                pltpu.make_async_copy(o_out.at[i], o_out.at[i], o_send.at[i]).wait()

            for h in range(PAIR):
                for st in range(2):
                    c = (i * PAIR + h) * 2 + st
                    total = mix_s[c, HEAD : HEAD + 1, :]
                    o_out[i, st * half : (st + 1) * half, h * HEAD : (h + 1) * HEAD] = (mix_s[c, :HEAD, :] * (1 / total)).T.astype(jnp.bfloat16)
            place = pl.ds(pl.multiple_of(me * TILE, TILE), TILE)

            @pl.when(away)
            def _():
                pltpu.make_async_remote_copy(o_out.at[i], o_in.at[p, :, place], o_send.at[i], o_recv.at[p],
                                             device_id={"sp": i}, device_id_type=MESH).start()

            @pl.when(jnp.logical_not(away))
            def _():
                o_in[p, :, place] = o_out[i]

        top_block = n - 1
        for hi in range(top_block, 1, -2):
            lo = hi - 1
            lax.fori_loop(0, lo, lambda j, _: (block((hi, j, False), (lo, j, False)), 0)[1], 0)
            block((hi, lo, False), (lo, lo, True))
            finish(lo)
            if hi != top_block:
                block((hi, hi, True))
                finish(hi)
        if n % 2 == 0:
            block((1, 0, False), (1, 1, True))
            finish(1)

        @pl.when(me != RELIEF)
        def _():
            block((top_block, top_block, True))

        @pl.when(me == RELIEF)
        def _():
            @pl.when(p > 0)
            def _():
                pltpu.make_async_copy(st_out, st_out, st_send).wait()

            for h in range(PAIR):
                for st in range(2):
                    c = (top_block * PAIR + h) * 2 + st
                    st_out[2 * h : 2 * h + 1, st * half : (st + 1) * half] = top_s[c : c + 1, :]
                    st_out[2 * h + 1 : 2 * h + 2, st * half : (st + 1) * half] = mix_s[c, HEAD : HEAD + 1, :]
            pltpu.make_async_remote_copy(st_out, st_in.at[p], st_send, st_recv.at[p], device_id={"sp": top_block}, device_id_type=MESH).start()

        finish(top_block)

    def corner(p, owners):
        pieces, scores, found = [], [], []
        for owner in owners:
            t = lax.rem(owner - me - 1 + n, n)
            q_at, k_at, v_at = lax.rem(p * n_qk + Q * n + t, 2 * n_qk), lax.rem(p * n_qk + K * n + t, 2 * n_qk), lax.rem(p * n_vt + t, 2 * n_vt)
            for h in range(PAIR):
                for st in range(2):
                    pieces.append((owner, v_at, h, st))
                    scores.append(_dot(qk_out[k_at, h, : half * (st + 1), :], qk_out[q_at, h, st * half : (st + 1) * half, :], 1, 1))
        weights = []
        for (owner, v_at, h, st), s in zip(pieces, scores):
            ok = lax.broadcasted_iota(jnp.int32, s.shape, 0) <= lax.broadcasted_iota(jnp.int32, s.shape, 1) + st * half
            s = jnp.where(ok, s, HIDDEN)
            top = s.max(axis=0, keepdims=True)
            weights.append((top, jnp.exp2((s - top) * e).astype(jnp.bfloat16)))
        for (owner, v_at, h, st), (top, w) in zip(pieces, weights):
            seen = w.shape[0]
            values = jnp.concatenate([vt_out[v_at, h, :, :seen], jnp.ones((8, seen), jnp.bfloat16)], axis=0)
            found.append((owner, h, st, top, _dot(values, w, 1, 0)))
        return found

    def corners(p):
        @pl.when(first_one)
        def _():
            def some(k, _):
                for owner, h, st, _top, mix in corner(p, [2 * k, 2 * k + 1]):
                    lanes = pl.ds(pl.multiple_of(owner * TILE + h * HEAD, HEAD), HEAD)
                    o_in[p, st * half : (st + 1) * half, lanes] = (mix[:HEAD] * (1 / mix[HEAD : HEAD + 1])).T.astype(jnp.bfloat16)
                return 0

            lax.fori_loop(0, n // 2, some, 0)

        @pl.when(last_one)
        def _():
            for owner, h, st, top, mix in corner(p, [RELIEF]):
                edge_top[p, h * 2 + st : h * 2 + st + 1, :] = top
                edge_mix[p, h * 2 + st] = mix

    def join(p):
        pltpu.make_async_copy(st_in.at[p], st_in.at[p], st_recv.at[p]).wait()
        for h in range(PAIR):
            for st in range(2):
                rows, lanes = slice(st * half, (st + 1) * half), slice(RELIEF * TILE + h * HEAD, RELIEF * TILE + (h + 1) * HEAD)
                c = h * 2 + st
                far_top, far_total = st_in[p, 2 * h : 2 * h + 1, rows], st_in[p, 2 * h + 1 : 2 * h + 2, rows]
                near_top, near = edge_top[p, c : c + 1, :], edge_mix[p, c]
                top = jnp.maximum(far_top, near_top)
                far_w, near_w = far_total * jnp.exp2((far_top - top) * e), jnp.exp2((near_top - top) * e)
                far = o_in[p, rows, lanes].astype(jnp.float32).T
                out = (far * far_w + near[:HEAD] * near_w) * (1 / (far_w + near[HEAD : HEAD + 1] * near_w))
                o_in[p, rows, lanes] = out.T.astype(jnp.bfloat16)

    def put(p):
        others = pl.ds(0, (n - 1) * TILE)

        @pl.when(jnp.logical_not(first_one))
        def _():
            pltpu.make_async_copy(o_in.at[p, :, others], o_in.at[p, :, others], o_recv.at[p]).wait()

        @pl.when(last_one)
        def _():
            join(p)

        def step(part, _):
            s = proj_steps + p * n + part
            slot = weights_here(s)

            for c in range(per_step):
                cols = pl.ds(pl.multiple_of((part * per_step + c) * TILE, TILE), TILE)
                acc[:, cols] += jnp.dot(o_in[p], wbuf[slot, c * n : (c + 1) * n].reshape(depth, TILE), preferred_element_type=jnp.float32)
            fetch(s + NW)

            @pl.when(p == pairs - 1)
            def _():
                cols = pl.ds(pl.multiple_of(part * per_step * TILE, TILE), per_step * TILE)
                a[:, cols] = acc[:, cols].astype(jnp.bfloat16)
                pltpu.make_async_copy(a.at[:, cols], y_ref.at[:, cols], y_sem).start()
            return 0

        lax.fori_loop(0, n, step, 0)

    late = min(3, pairs)

    def turn(p, _):
        @pl.when(p < pairs)
        def _():
            lax.fori_loop(0, n_qk, lambda t, _: (project_qk(p, t), 0)[1], 0)
            project_qk(p, jnp.int32(n_qk), flush=True)

            def one(t, _):
                @pl.when((p > 0) & (t == tiles - 1))
                def _():
                    load_pair(p - 1)
                project_vt(p, t)
                return 0

            lax.fori_loop(n_qk, tiles, one, 0)
            project_vt(p, jnp.int32(tiles), flush=True)
            corners(p)

        first = jnp.where(p == pairs + 1, pairs - late, 0)
        last = jnp.where(p < pairs, 0, jnp.where(p == pairs, pairs - late, pairs))

        lax.fori_loop(first, last, lambda k, _: (put(k), 0)[1], 0)

        @pl.when(p == pairs)
        def _():
            load_pair(p - 1)

        @pl.when((p > 0) & (p <= pairs))
        def _():
            attend(p - 1)
        return 0

    lax.fori_loop(0, pairs + 2, turn, 0)

    pltpu.make_async_copy(a, y_ref, y_sem).wait()
    for slot in range(2 * n_qk):
        if slot % n != n - 1:
            @pl.when(jnp.logical_not(stays_here(slot % n_qk // n, owner_of(slot))))
            def _():
                pltpu.make_async_copy(qk_out.at[slot], qk_out.at[slot], qk_send.at[slot]).wait()
    for slot in range(2 * n_vt):
        if slot % n != n - 1:
            @pl.when(jnp.logical_not(stays_here(2, owner_of(slot))))
            def _():
                pltpu.make_async_copy(vt_out.at[slot], vt_out.at[slot], vt_send.at[slot]).wait()

    @pl.when(me == RELIEF)
    def _():
        pltpu.make_async_copy(st_out, st_out, st_send).wait()

    for i in range(1, n):
        @pl.when(i != me)
        def _():
            pltpu.make_async_copy(o_out.at[i], o_out.at[i], o_send.at[i]).wait()


def solution(mesh):
    n = mesh.shape["sp"]

    def step(x, gain, wq, wk, wv, wo):
        own, d = x.shape
        heads = wq.shape[1] // HEAD
        pairs = heads // n // PAIR
        seq = n * own
        place = lax.axis_index("sp") * own + jnp.arange(own)
        angle = place.astype(jnp.float32)[:, None] * THETA ** (-jnp.arange(HEAD // 2, dtype=jnp.float32) / (HEAD // 2))
        cos, sin = jnp.cos(angle), jnp.sin(angle)
        bf16, f32, dma = jnp.bfloat16, jnp.float32, pltpu.SemaphoreType.DMA
        vmem, hbm = pl.BlockSpec(memory_space=pltpu.VMEM), pl.BlockSpec(memory_space=pl.ANY)
        flops = 2 * own * d * 4 * heads * HEAD + 2 * heads // n * seq * seq * HEAD
        y, _, _ = pl.pallas_call(
            functools.partial(_kernel, n, pairs),
            out_shape=[jax.ShapeDtypeStruct((own, d), bf16), jax.ShapeDtypeStruct((pairs, 2, PAIR, seq, HEAD), bf16),
                       jax.ShapeDtypeStruct((pairs, PAIR, HEAD, seq), bf16)],
            in_specs=[hbm, vmem, vmem, vmem, hbm, hbm, hbm, hbm],
            out_specs=[hbm, hbm, hbm],
            scratch_shapes=[
                pltpu.VMEM((own, d), bf16),
                pltpu.VMEM((own, d), f32),
                pltpu.VMEM((NW, d // TILE, TILE, TILE), bf16),
                pltpu.VMEM((4 * n + 1, PAIR, own, HEAD), bf16),
                pltpu.VMEM((2 * n + 1, PAIR, HEAD, own), bf16),
                pltpu.VMEM((n, own, TILE), bf16),
                pltpu.VMEM((pairs, own, n * TILE), bf16),
                pltpu.VMEM((2, PAIR, seq, HEAD), bf16),
                pltpu.VMEM((PAIR, HEAD, seq), bf16),
                pltpu.VMEM((own, TILE), bf16),
                pltpu.VMEM((own, HEAD), f32),
                pltpu.VMEM((own, HEAD), f32),
                pltpu.VMEM((2 * n * PAIR, own // 2), f32),
                pltpu.VMEM((2 * n * PAIR, HEAD + 8, own // 2), f32),
                pltpu.VMEM((8, own), f32),
                pltpu.VMEM((pairs, 8, own), f32),
                pltpu.VMEM((pairs, 8, own // 2), f32),
                pltpu.VMEM((pairs, 2 * PAIR, HEAD + 8, own // 2), f32),
                dma((NW,)), dma(()), dma(()), dma((2,)), dma((4 * n,)), dma((2 * n,)), dma((n,)), dma(()), dma((pairs,)), dma((pairs,)), dma((pairs,)),
                dma((pairs,)), dma((pairs,)),
            ],
            compiler_params=pltpu.CompilerParams(collective_id=0, has_side_effects=True, vmem_limit_bytes=66 * 10**6),
            cost_estimate=pl.CostEstimate(flops=flops, transcendentals=heads // n * seq * seq // 2, bytes_accessed=2 * 4 * d * d),
            name="attention_half",
        )(x, gain[None], cos, sin, *(w.reshape(d // TILE, TILE, -1) for w in (wq, wk, wv)),
          wo.reshape(n, pairs, TILE, d))
        return y

    tokens, whole = P(("dp", "sp"), None), P(None, None)
    return jax.shard_map(step, mesh=mesh, in_specs=(tokens, P(None), whole, whole, whole, whole), out_specs=tokens, check_vma=False)
```
